64 devices in a mesh: rep: 4 (over x, y), dp: 16 (over z, core).
Axes of the slice: x: 2, y: 2, z: 8, core: 2. Of those that a mesh axis runs over, the one named last changes fastest.
The devices are a block of a 4x4x8 slice.
Arguments:
- x: bfloat16 [64, 2048, 512], P(('rep', 'dp')), parts along dimension 0
- dy: bfloat16 [64, 2048, 512], P(('rep', 'dp')), parts along dimension 0
- wq: bfloat16 [2, 512, 1024], P(None, 'dp')
- wk: bfloat16 [2, 512, 512], P(None, 'dp')
- wv: bfloat16 [2, 512, 512], P(None, 'dp')
- wo: bfloat16 [2, 1024, 512], P(None, 'dp')
- w_gate: bfloat16 [2, 512, 1536], P(None, 'dp')
- w_up: bfloat16 [2, 512, 1536], P(None, 'dp')
- w_down: bfloat16 [2, 1536, 512], P(None, 'dp')
Outputs:
- output 1: bfloat16 [64, 2048, 512], P(('rep', 'dp')), parts along dimension 0
- output 2: bfloat16 [8, 512, 1024], P('rep', 'dp'), parts along dimension 0
- output 3: bfloat16 [8, 512, 512], P('rep', 'dp'), parts along dimension 0
- output 4: bfloat16 [8, 512, 512], P('rep', 'dp'), parts along dimension 0
- output 5: bfloat16 [8, 1024, 512], P('rep', 'dp'), parts along dimension 0
- output 6: bfloat16 [8, 512, 1536], P('rep', 'dp'), parts along dimension 0
- output 7: bfloat16 [8, 512, 1536], P('rep', 'dp'), parts along dimension 0
- output 8: bfloat16 [8, 1536, 512], P('rep', 'dp'), parts along dimension 0
There are 4 independent parts. The reference program is written for one: setup_inputs(seed, part) draws one part's arguments, and reference() takes and returns one part's arrays. A program takes and returns all parts, laid end to end along the dimension named above; an argument that names none is the same for every part.
All inputs are finite; a program needn't handle non-finite values.
Results may differ from the reference program's by a relative error of at most 0.0311.
Values are sent between devices in bfloat16 or wider.
A program may use at most 768 MiB of HBM per device.

```python
import jax
import jax.numpy as jnp
from jax import lax

SEQUENCES = 16
TOKENS = 2048
D = 512
HEADS = 8
KV_HEADS = 4
HEAD = 128
FF = 1536
LAYERS = 2
THETA = 10000
NAMES = ("wq", "wk", "wv", "wo", "w_gate", "w_up", "w_down")
SHAPES = {
    "wq": (LAYERS, D, HEADS * HEAD),
    "wk": (LAYERS, D, KV_HEADS * HEAD),
    "wv": (LAYERS, D, KV_HEADS * HEAD),
    "wo": (LAYERS, HEADS * HEAD, D),
    "w_gate": (LAYERS, D, FF),
    "w_up": (LAYERS, D, FF),
    "w_down": (LAYERS, FF, D),
}


def bump(key, n, height):
    away = (jnp.arange(n, dtype=jnp.int32) - jax.random.randint(key, (), 0, n, jnp.int32)) % n
    return jnp.where(away < n // 8, height, 1.0)


def together(key, own, strength):
    shared = jax.random.normal(key, own.shape[1:], jnp.float32)
    return (own + strength * shared) * lax.rsqrt(1 + strength * strength)


def setup_inputs(seed: int = 0, part: int = 0) -> dict:
    kx, kdy, ka, kb, kz, kf, kh, kl, *keys = jax.random.split(jax.random.key(seed), 8 + 3 * len(NAMES))
    kx, kdy, ka, kb = (jax.random.fold_in(k, part) for k in (kx, kdy, ka, kb))
    kw, km, kv = (keys[i::3] for i in range(3))
    shape = (SEQUENCES, TOKENS, D)
    much_x, much_dy = jax.random.uniform(kz, (2,), jnp.float32, 0.0, 1.0)
    loud = 2.0 ** jax.random.uniform(jax.random.fold_in(kz, 1), (), jnp.float32, -1.0, 2.0)
    layers = 2.0 ** jax.random.uniform(kl, (LAYERS, 1, 1), jnp.float32, -1.0, 1.0)
    times = {"wq": 1.0, "wk": 1.0, "wv": 2.0, "wo": layers, "w_gate": 1.0, "w_up": bump(kh, FF, 4.0), "w_down": layers}
    x = together(ka, jax.random.normal(kx, shape, jnp.float32), much_x) * bump(kf, D, 4.0)
    dy = together(kb, jax.random.normal(kdy, shape, jnp.float32), much_dy)
    drawn = {"x": x.astype(jnp.bfloat16), "dy": (loud * dy * (SEQUENCES * TOKENS) ** -0.5).astype(jnp.bfloat16)}
    for key, name in zip(kw, NAMES, strict=True):
        drawn[name] = (jax.random.normal(key, SHAPES[name], jnp.float32) * SHAPES[name][1] ** -0.5 * times[name]).astype(jnp.bfloat16)
    return drawn


def matmul(a, w):
    return jnp.dot(a, w, preferred_element_type=jnp.float32).astype(jnp.bfloat16)


def normed(h):
    wide = h.astype(jnp.float32)
    scale = lax.rsqrt(jnp.mean(wide**2, -1, keepdims=True) + 1e-6)
    return (wide * scale).astype(jnp.bfloat16)


def turned(t, theta):
    half = t.shape[-1] // 2
    angle = jnp.arange(t.shape[0], dtype=jnp.float32)[:, None] * theta ** (-jnp.arange(half, dtype=jnp.float32) / half)
    cos, sin = jnp.cos(angle)[:, None], jnp.sin(angle)[:, None]
    a, b = t[..., :half].astype(jnp.float32), t[..., half:].astype(jnp.float32)
    return jnp.concatenate([a * cos - b * sin, b * cos + a * sin], -1).astype(jnp.bfloat16)


def seen_by(q, k, v):
    tokens, kv = q.shape[0], k.shape[1]
    q = q.reshape(tokens, kv, -1, q.shape[-1])
    scores = jnp.einsum("tgsd,ugd->gstu", q.astype(jnp.float32), k.astype(jnp.float32)) * q.shape[-1] ** -0.5
    place = jnp.arange(tokens)
    weights = jax.nn.softmax(jnp.where(place[:, None] >= place, scores, -jnp.inf), -1).astype(jnp.bfloat16)
    return jnp.einsum("gstu,ugd->tgsd", weights.astype(jnp.float32), v.astype(jnp.float32)).astype(jnp.bfloat16).reshape(tokens, -1)


def layer(h, w):
    a = normed(h)
    q, k = (turned(matmul(a, w[name]).reshape(h.shape[0], -1, HEAD), THETA) for name in ("wq", "wk"))
    h = h + matmul(seen_by(q, k, matmul(a, w["wv"]).reshape(h.shape[0], -1, HEAD)), w["wo"])
    b = normed(h)
    gate = jnp.dot(b, w["w_gate"], preferred_element_type=jnp.float32)
    up = jnp.dot(b, w["w_up"], preferred_element_type=jnp.float32)
    return h + matmul((jax.nn.silu(gate) * up).astype(jnp.bfloat16), w["w_down"])


def stack(weights, h):
    return lax.scan(lambda h, w: (layer(h, w), None), h, weights)[0]


def reference(x, dy, wq, wk, wv, wo, w_gate, w_up, w_down):
    weights = dict(zip(NAMES, (wq, wk, wv, wo, w_gate, w_up, w_down), strict=True))

    def take(so_far, sequence):
        h, by_y = sequence
        _, back = jax.vjp(stack, weights, h)
        by_weights, by_h = back(by_y)
        return jax.tree.map(lambda total, term: total + term.astype(jnp.float32), so_far, by_weights), by_h

    none_yet = {name: jnp.zeros(w.shape, jnp.float32) for name, w in weights.items()}
    by_weights, by_x = lax.scan(take, none_yet, (x, dy))
    return (by_x, *(by_weights[name].astype(jnp.bfloat16) for name in NAMES))
```

```python
import functools

import jax
import jax.numpy as jnp
from jax import lax
from jax.experimental import pallas as pl
from jax.experimental.pallas import tpu as pltpu
from jax.sharding import PartitionSpec as P

HEAD = 128
THETA = 10000
HIDDEN = -2e30
LOW = -1e30
LOG2E = 1.4426950408889634
VMEM = 56 * 2**20
BF, F32 = jnp.bfloat16, jnp.float32


def dot(a, b, ca=1, cb=0):
    return lax.dot_general(a, b, (((ca,), (cb,)), ((), ())), preferred_element_type=F32)


def flat(ref):
    n, rows, columns = ref.shape
    return ref[...].reshape(n * rows, columns)


def norm(h):
    wide = h.astype(F32)
    scale = lax.rsqrt(jnp.mean(wide * wide, -1, keepdims=True) + 1e-6)
    return wide, scale, (wide * scale).astype(BF)


def norm_back(wide, scale, by):
    by = by.astype(BF).astype(F32)
    inner = jnp.mean(by * wide, -1, keepdims=True)
    return (scale * by - (scale * scale * scale) * inner * wide).astype(BF).astype(F32)


def params(*semantics):
    return pltpu.CompilerParams(dimension_semantics=semantics, vmem_limit_bytes=VMEM)


def cost(flops, nbytes, exps=0):
    return pl.CostEstimate(flops=int(flops), bytes_accessed=int(nbytes), transcendentals=int(exps))


def whole(shape):
    return pl.BlockSpec(shape, lambda *_: (0,) * len(shape))


def shape(dims, dtype=BF):
    return jax.ShapeDtypeStruct(dims, dtype)


def qkv_kernel(h_ref, w_ref, cos_ref, sin_ref, q_ref, k_ref, v_ref):
    _, _, a = norm(h_ref[...])
    kv, g = q_ref.shape[:2]
    cos, sin = cos_ref[...], sin_ref[...]

    def turned(t):
        t = t.astype(F32)
        return (t * cos + pltpu.roll(t, HEAD // 2, 1) * sin).astype(BF)

    t = dot(a, w_ref[...]).astype(BF)
    heads = [t[:, i * HEAD : (i + 1) * HEAD] for i in range(kv * (g + 2))]
    for i in range(kv):
        for n in range(g):
            q_ref[i, n] = turned(heads[i * g + n])
        k_ref[i] = turned(heads[kv * g + i])
        v_ref[i] = heads[kv * (g + 1) + i]


def qkv_of(h, w, cos, sin, kv, g, tb=512):
    t, d = h.shape
    rows = pl.BlockSpec((tb, d), lambda i: (i, 0))
    table = pl.BlockSpec((tb, HEAD), lambda i: (i, 0))
    key = pl.BlockSpec((kv, tb, HEAD), lambda i: (0, i, 0))
    return pl.pallas_call(
        qkv_kernel,
        grid=(t // tb,),
        in_specs=[rows, whole(w.shape), table, table],
        out_specs=[pl.BlockSpec((kv, g, tb, HEAD), lambda i: (0, 0, i, 0)), key, key],
        out_shape=[shape((kv, g, t, HEAD)), shape((kv, t, HEAD)), shape((kv, t, HEAD))],
        compiler_params=params("arbitrary"),
        cost_estimate=cost(2 * t * w.size, 2 * (h.size + w.size + t * w.shape[1]) + 8 * cos.size),
        name="qkv",
    )(h, w, cos, sin)


def qkv_back_kernel(dq_ref, dk_ref, dv_ref, h_ref, dh_ref, w_ref, cos_ref, sin_ref, out_ref, dw_ref, dw_s):
    kv, g = dq_ref.shape[:2]
    wide, scale, a = norm(h_ref[...])
    cos, sin = cos_ref[...], sin_ref[...]

    def back(t):
        t = t.astype(F32)
        return (t * cos - pltpu.roll(t, HEAD // 2, 1) * sin).astype(BF)

    @pl.when(pl.program_id(0) == 0)
    def _():
        dw_s[...] = jnp.zeros_like(dw_s)

    parts = [back(dq_ref[i, n]) for i in range(kv) for n in range(g)] + [back(dk_ref[i]) for i in range(kv)] + [dv_ref[i] for i in range(kv)]
    by = jnp.concatenate(parts, axis=1)
    dw_s[...] += dot(a, by, 0, 0)
    by_a = dot(by, w_ref[...], 1, 1)
    out_ref[...] = (dh_ref[...].astype(F32) + norm_back(wide, scale, by_a)).astype(BF)

    @pl.when(pl.program_id(0) == pl.num_programs(0) - 1)
    def _():
        dw_ref[...] = dw_s[...].astype(BF)


def qkv_back(dq, dk, dv, h, dh, w, cos, sin, tb=512):
    t, d = h.shape
    kv, g = dq.shape[:2]
    rows = pl.BlockSpec((tb, d), lambda i: (i, 0))
    table = pl.BlockSpec((tb, HEAD), lambda i: (i, 0))
    key = pl.BlockSpec((kv, tb, HEAD), lambda i: (0, i, 0))
    return pl.pallas_call(
        qkv_back_kernel,
        grid=(t // tb,),
        in_specs=[pl.BlockSpec((kv, g, tb, HEAD), lambda i: (0, 0, i, 0)), key, key, rows, rows, whole(w.shape), table, table],
        out_specs=[rows, whole(w.shape)],
        out_shape=[shape((t, d)), shape(w.shape)],
        scratch_shapes=[pltpu.VMEM(w.shape, F32)],
        compiler_params=params("arbitrary"),
        cost_estimate=cost(4 * t * w.size, 2 * (3 * h.size + 2 * w.size + t * w.shape[1]) + 8 * cos.size),
        name="qkv_back",
    )(dq, dk, dv, h, dh, w, cos, sin)


def attend_kernel(q_ref, k_ref, v_ref, o_ref, lse_ref, top_s, mix_s, *, e, bk):
    kv, g, bq, d = q_ref.shape
    iq = pl.program_id(0)
    heads = [(i, n) for i in range(kv) for n in range(g)]
    top_s[...] = jnp.full_like(top_s, LOW)
    mix_s[...] = jnp.zeros_like(mix_s)

    def block(first, keys, at, masked):
        here = pl.ds(first, keys)
        wide = bq - at
        ones = jnp.ones((8, keys), BF)
        scores = [dot(k_ref[i, here, :], q_ref[i, n, at:, :], 1, 1) for i, n in heads]
        if masked:
            ok = lax.broadcasted_iota(jnp.int32, (keys, wide), 1) >= lax.broadcasted_iota(jnp.int32, (keys, wide), 0)
        weights, keeps = [], []
        for m, s in enumerate(scores):
            if masked:
                s = jnp.where(ok, s, HIDDEN)
            old = top_s[m : m + 1, at:]
            top = jnp.maximum(old, s.max(axis=0, keepdims=True))
            top_s[m : m + 1, at:] = top
            weights.append(jnp.exp2((s - top) * e).astype(BF))
            keeps.append(jnp.exp2((old - top) * e))
        for m, (i, n) in enumerate(heads):
            values = jnp.concatenate([v_ref[i, here, :].T, ones], axis=0)
            mix_s[m, :, at:] = mix_s[m, :, at:] * keeps[m] + dot(values, weights[m])

    lax.fori_loop(0, iq * (bq // bk), lambda j, _: block(pl.multiple_of(j * bk, bk), bk, 0, False), None)
    half = bq // 2
    block(pl.multiple_of(iq * bq, bq), half, 0, True)
    block(pl.multiple_of(iq * bq + half, half), half, half, True)
    for m, (i, n) in enumerate(heads):
        total = mix_s[m, d : d + 1, :]
        o_ref[:, m * d : (m + 1) * d] = (mix_s[m, :d, :] * (1 / total)).T.astype(BF)
        lse_ref[m : m + 1, :] = top_s[m : m + 1, :] * e + jnp.log2(total)


def attend(q, k, v, bq=512, bk=512):
    kv, g, t, d = q.shape
    keys = whole(k.shape)
    return pl.pallas_call(
        functools.partial(attend_kernel, e=d**-0.5 * LOG2E, bk=bk),
        grid=(t // bq,),
        in_specs=[pl.BlockSpec((kv, g, bq, d), lambda i: (0, 0, i, 0)), keys, keys],
        out_specs=[pl.BlockSpec((bq, kv * g * d), lambda i: (i, 0)), pl.BlockSpec((kv * g, bq), lambda i: (0, i))],
        out_shape=[shape((t, kv * g * d)), shape((kv * g, t), F32)],
        scratch_shapes=[pltpu.VMEM((kv * g, bq), F32), pltpu.VMEM((kv * g, d + 8, bq), F32)],
        compiler_params=params("arbitrary"),
        cost_estimate=cost(4 * kv * g * t * t * d, 2 * (2 * q.size + 2 * k.size), kv * g * t * t // 2),
        name="attend",
    )(q, k, v)


def attend_back_kernel(q_ref, k_ref, v_ref, do_ref, lse_ref, delta_ref, dq_ref, dk_ref, dv_ref, dq_s, dk_s, dv_s, *, scale, bk):
    kv, g, bq, d = q_ref.shape
    iq = pl.program_id(0)
    e = scale * LOG2E
    cols = g * bq

    @pl.when(iq == 0)
    def _():
        dk_s[...] = jnp.zeros_like(dk_s)
        dv_s[...] = jnp.zeros_like(dv_s)

    dq_s[...] = jnp.zeros_like(dq_s)

    def row(ref, i):
        return jnp.concatenate([ref[i * g + n : i * g + n + 1, :] for n in range(g)], axis=1)

    lses = [row(lse_ref, i) for i in range(kv)]
    deltas = [row(delta_ref, i) for i in range(kv)]

    def block(first, keys, masked):
        here = pl.ds(first, keys)
        qs = [q_ref[i].reshape(cols, d) for i in range(kv)]
        dos = [do_ref[i].reshape(cols, d) for i in range(kv)]
        scores = [dot(k_ref[i, here, :], qs[i], 1, 1) for i in range(kv)]
        dps = [dot(v_ref[i, here, :], dos[i], 1, 1) for i in range(kv)]
        if masked:
            ok = lax.rem(lax.broadcasted_iota(jnp.int32, (keys, cols), 1), bq) >= lax.broadcasted_iota(jnp.int32, (keys, cols), 0)
        for i in range(kv):
            p = jnp.exp2(scores[i] * e - lses[i])
            if masked:
                p = jnp.where(ok, p, 0.0)
            ds = (p * (dps[i] - deltas[i])).astype(BF)
            dv_s[i, here, :] += dot(p.astype(BF), dos[i])
            dk_s[i, here, :] += dot(ds, qs[i])
            dq_s[i] += dot(k_ref[i, here, :].T, ds)

    most = lax.div(iq * bq, bk)
    lax.fori_loop(0, most, lambda j, _: block(pl.multiple_of(j * bk, bk), bk, False), None)
    lax.fori_loop(most * (bk // bq), iq, lambda j, _: block(pl.multiple_of(j * bq, bq), bq, False), None)
    block(pl.multiple_of(iq * bq, bq), bq, True)
    for i in range(kv):
        dq_ref[i] = (dq_s[i] * scale).T.reshape(g, bq, d).astype(BF)

    @pl.when(iq == pl.num_programs(0) - 1)
    def _():
        dk_ref[...] = (dk_s[...] * scale).astype(BF)
        dv_ref[...] = dv_s[...].astype(BF)


def attend_back(q, k, v, do, lse, delta, bq=256, bk=512):
    kv, g, t, d = q.shape
    queries = pl.BlockSpec((kv, g, bq, d), lambda i: (0, 0, i, 0))
    keys, stats = whole(k.shape), pl.BlockSpec((kv * g, bq), lambda i: (0, i))
    return pl.pallas_call(
        functools.partial(attend_back_kernel, scale=d**-0.5, bk=bk),
        grid=(t // bq,),
        in_specs=[queries, keys, keys, queries, stats, stats],
        out_specs=[queries, keys, keys],
        out_shape=[shape(q.shape), shape(k.shape), shape(k.shape)],
        scratch_shapes=[pltpu.VMEM((kv, d, g * bq), F32), pltpu.VMEM(k.shape, F32), pltpu.VMEM(k.shape, F32)],
        compiler_params=params("arbitrary"),
        cost_estimate=cost(10 * kv * g * t * t * d, 2 * (3 * q.size + 4 * k.size), kv * g * t * t // 2),
        name="attend_back",
    )(q, k, v, do, lse, delta)


def pack(wo, wg, wu, wd):
    d = wo.shape[1]
    cut = lambda w: [w[:, i : i + d] for i in range(0, w.shape[1], d)]
    gates, ups = cut(wg), cut(wu)
    return jnp.concatenate([wo, gates[0], wd, *gates[1:], *ups], axis=0)


def places(ro, rd, rg, pieces):
    rest = ro + rg + rd
    gates = [ro] + [rest + i * rg for i in range(pieces - 1)]
    ups = [rest + (pieces - 1 + i) * rg for i in range(pieces)]
    return 0, ro + rg, gates, ups


def unpack(packed, ro, rd, rg, pieces):
    o, dn, gates, ups = places(ro, rd, rg, pieces)
    join = lambda at: jnp.concatenate([packed[a : a + rg] for a in at], axis=1)
    return packed[o : o + ro], join(gates), join(ups), packed[dn : dn + rd]


def weight_specs(n, d, ro, rd, rg, pieces):
    o, dn, gates, ups = places(ro, rd, rg, pieces)

    def spec(rows, at):
        block = at // rows
        return pl.BlockSpec((n, rows, d), lambda *_: (0, block, 0))

    return [spec(ro, o), spec(rd, dn)] + [spec(rg, a) for a in gates + ups]


def mlp_kernel(o_ref, h_ref, wo_ref, wd_ref, *rest, pieces):
    gates, ups, out_ref = rest[:pieces], rest[pieces : 2 * pieces], rest[-1]
    d = h_ref.shape[1]
    h1 = (h_ref[...].astype(F32) + dot(o_ref[...], flat(wo_ref)).astype(BF).astype(F32)).astype(BF)
    _, _, b = norm(h1)
    down = flat(wd_ref)
    total = None
    for j in range(pieces):
        gate, up = dot(b, flat(gates[j])), dot(b, flat(ups[j]))
        act = (gate * jax.nn.sigmoid(gate) * up).astype(BF)
        term = dot(act, down[j * d : (j + 1) * d])
        total = term if total is None else total + term
    out_ref[...] = (h1.astype(F32) + total.astype(BF).astype(F32)).astype(BF)


def mlp(o, h, w, sizes, tb=512):
    t, d = h.shape
    rows = pl.BlockSpec((tb, d), lambda i: (i, 0))
    specs = weight_specs(w.shape[0], d, *sizes)
    return pl.pallas_call(
        functools.partial(mlp_kernel, pieces=sizes[-1]),
        grid=(t // tb,),
        in_specs=[pl.BlockSpec((tb, o.shape[1]), lambda i: (i, 0)), rows, *specs],
        out_specs=rows,
        out_shape=shape((t, d)),
        compiler_params=params("arbitrary"),
        cost_estimate=cost(2 * t * w.size, 2 * (o.size + 2 * h.size + w.size)),
        name="mlp",
    )(o, h, *[w] * len(specs))


def mlp_back_kernel(o_ref, h_ref, dy_ref, wo_ref, wd_ref, *rest, pieces, sizes):
    gates, ups = rest[:pieces], rest[pieces : 2 * pieces]
    dh_ref, do_ref, delta_ref, dw_ref, dwo_s, dwd_s, dwg_s, dwu_s = rest[2 * pieces :]
    d = h_ref.shape[1]
    kv, g, tb, _ = do_ref.shape
    step = pl.program_id(0)

    @pl.when(step == 0)
    def _():
        for s in (dwo_s, dwd_s, dwg_s, dwu_s):
            s[...] = jnp.zeros_like(s)

    o, dy = o_ref[...], dy_ref[...]
    wo, down = flat(wo_ref), flat(wd_ref)
    h1 = (h_ref[...].astype(F32) + dot(o, wo).astype(BF).astype(F32)).astype(BF)
    wide, scale, b = norm(h1)
    by_b = jnp.zeros((tb, d), F32)
    for j in range(pieces):
        wg, wu, wd = flat(gates[j]), flat(ups[j]), down[j * d : (j + 1) * d]
        gate, up = dot(b, wg), dot(b, wu)
        by_act = dot(dy, wd, 1, 1).astype(BF).astype(F32)
        sig = jax.nn.sigmoid(gate)
        silu = gate * sig
        act = (silu * up).astype(BF)
        by_gate = (by_act * up * (sig + silu * (1 - sig))).astype(BF)
        by_up = (by_act * silu).astype(BF)
        dwd_s[j * d : (j + 1) * d, :] += dot(act, dy, 0, 0)
        dwg_s[j] += dot(b, by_gate, 0, 0)
        dwu_s[j] += dot(b, by_up, 0, 0)
        by_b += dot(by_gate, wg, 1, 1) + dot(by_up, wu, 1, 1)
    dh = (dy.astype(F32) + norm_back(wide, scale, by_b)).astype(BF)
    dh_ref[...] = dh
    by_o = dot(dh, wo, 1, 1).astype(BF)
    dwo_s[...] += dot(o, dh, 0, 0)
    heads = kv * g
    for m in range(heads):
        do_ref[m // g, m % g] = by_o[:, m * HEAD : (m + 1) * HEAD]
    both = by_o.astype(F32) * o.astype(F32)
    high = both.astype(BF)
    low = (both - high.astype(F32)).astype(BF)
    pick = (lax.broadcasted_iota(jnp.int32, (heads, heads * HEAD), 1) // HEAD == lax.broadcasted_iota(jnp.int32, (heads, heads * HEAD), 0)).astype(F32).astype(BF)
    delta_ref[...] = dot(pick, high, 1, 1) + dot(pick, low, 1, 1)

    @pl.when(step == pl.num_programs(0) - 1)
    def _():
        n = dw_ref.shape[0]
        ro, rd, rg, _ = sizes
        at_o, at_d, at_g, at_u = places(*sizes)
        dw_ref[:, at_o : at_o + ro, :] = dwo_s[...].astype(BF).reshape(n, ro, d)
        dw_ref[:, at_d : at_d + rd, :] = dwd_s[...].astype(BF).reshape(n, rd, d)
        for j in range(pieces):
            dw_ref[:, at_g[j] : at_g[j] + rg, :] = dwg_s[j].astype(BF).reshape(n, rg, d)
            dw_ref[:, at_u[j] : at_u[j] + rg, :] = dwu_s[j].astype(BF).reshape(n, rg, d)


def mlp_back(o, h, dy, w, sizes, kv, g, tb=512):
    t, d = h.shape
    heads = kv * g
    pieces = sizes[-1]
    rows = pl.BlockSpec((tb, d), lambda i: (i, 0))
    specs = weight_specs(w.shape[0], d, *sizes)
    return pl.pallas_call(
        functools.partial(mlp_back_kernel, pieces=pieces, sizes=sizes),
        grid=(t // tb,),
        in_specs=[pl.BlockSpec((tb, o.shape[1]), lambda i: (i, 0)), rows, rows, *specs],
        out_specs=[rows, pl.BlockSpec((kv, g, tb, HEAD), lambda i: (0, 0, i, 0)), pl.BlockSpec((heads, tb), lambda i: (0, i)), whole(w.shape)],
        out_shape=[shape((t, d)), shape((kv, g, t, HEAD)), shape((heads, t), F32), shape(w.shape)],
        scratch_shapes=[pltpu.VMEM((heads * HEAD, d), F32), pltpu.VMEM((pieces * d, d), F32), pltpu.VMEM((pieces, d, d), F32),
                        pltpu.VMEM((pieces, d, d), F32)],
        compiler_params=params("arbitrary"),
        cost_estimate=cost(8 * t * w.size, 2 * (2 * o.size + 4 * h.size + 2 * w.size), t * pieces * d),
        name="mlp_back",
    )(o, h, dy, *[w] * len(specs))


def solution(mesh):
    n = mesh.shape["dp"]

    def step(x, dy, wq, wk, wv, wo, wg, wu, wd):
        layers, d = wq.shape[0], x.shape[2]
        kv = wk.shape[2] // HEAD
        g = wq.shape[2] // HEAD // kv
        sizes = (wo.shape[1], wd.shape[1], wg.shape[1], wg.shape[2] // d)
        first, second = [], []
        for i in range(layers):
            first.append(lax.all_gather(jnp.concatenate([wq[i], wk[i], wv[i]], axis=1), "dp", axis=0, tiled=True))
            second.append(lax.all_gather(pack(wo[i], wg[i], wu[i], wd[i]), "dp", axis=0))
        half = HEAD // 2
        angle = jnp.arange(x.shape[1], dtype=F32)[:, None] * THETA ** (-jnp.arange(half, dtype=F32) / half)
        cos, sin = jnp.cos(angle), jnp.sin(angle)
        cos, sin = jnp.concatenate([cos, cos], 1), jnp.concatenate([-sin, sin], 1)

        h, kept = x[0], []
        for i in range(layers):
            q, k, v = qkv_of(h, first[i], cos, sin, kv, g)
            o, lse = attend(q, k, v)
            kept.append((h, q, k, v, o, lse))
            if i < layers - 1:
                h = mlp(o, h, second[i], sizes)
        by_h, mine = dy[0], [None] * layers
        for i in reversed(range(layers)):
            h, q, k, v, o, lse = kept[i]
            by_h, do, delta, dw = mlp_back(o, h, by_h, second[i], sizes, kv, g)
            d_out, d_gate, d_up, d_down = unpack(lax.psum_scatter(dw, "dp", scatter_dimension=0), *sizes)
            dq, dk, dv = attend_back(q, k, v, do, lse, delta)
            by_h, dw = qkv_back(dq, dk, dv, h, by_h, first[i], cos, sin)
            dw = lax.psum_scatter(dw, "dp", scatter_dimension=0, tiled=True)
            cuts = [wq.shape[2], wq.shape[2] + wk.shape[2]]
            mine[i] = [*jnp.split(dw, cuts, axis=1), d_out, d_gate, d_up, d_down]
        return (by_h[None], *(jnp.stack([mine[i][m] for i in range(layers)]) for m in range(7)))

    states, cut = P(("rep", "dp"), None, None), P(None, "dp", None)
    return jax.shard_map(
        step,
        mesh=mesh,
        in_specs=(states, states) + (cut,) * 7,
        out_specs=(states,) + (P("rep", "dp", None),) * 7,
        check_vma=False,
    )
```
